32 devices in a mesh: section: 2 (over y), row: 4 (over x, core), col: 4 (over z).
Axes of the slice: x: 2, y: 2, z: 4, core: 2. Of those that a mesh axis runs over, the one named last changes fastest.
Arguments:
- inputs: float32 [3, 128, 16384], P(None, None, ('row', 'col')), may hold values from -512 to 512
- weights: float32 [2, 4, 4, 1024, 16384], P('section', None, 'col', None, 'row'), may hold values from -1 to 1
- norm_gain: float32 [2, 16384], P('section', ('row', 'col')), may hold values from 0.5 to 1.5
Outputs:
- section_outputs: float32 [2, 3, 128, 16384], P('section', None, None, ('row', 'col'))
The draws below stay inside these ranges and needn't reach their ends.
All inputs are finite; a program needn't handle non-finite values.
Results may differ from the reference program's by a relative error of at most 0.00036.
Values sent between devices are 32-bit elements; how exact they have to be, the bound alone decides.
A program may use at most 192 MiB of HBM per device.

```python
import math
import jax
import jax.numpy as jnp
from jax import lax

D = 16384
B = 128
M = 3
LAYERS = 2
ROW_BLOCKS = 4
COL_BLOCKS = 4
PIECE = 1024


offset_scale = 64.0


def shared_basis(key):
    raw_draw = jax.random.normal(jax.random.fold_in(key, 7103), (D, M * B), jnp.float32)
    basis_cols, upper_part = jnp.linalg.qr(raw_draw)
    return basis_cols


def draw_inputs(key, part):
    basis_cols = shared_basis(key)
    count = M * B
    mixing = jax.random.normal(jax.random.fold_in(key, 211), (count, count), jnp.float32) / math.sqrt(count)
    amplitude = jnp.ones((count, 1), jnp.float32)
    rough = jax.random.normal(jax.random.fold_in(key, 229), (count, D), jnp.float32)
    along = jnp.dot(mixing, basis_cols.T, precision=lax.Precision.HIGHEST)
    large = offset_scale * math.sqrt(D) * amplitude * along
    values = jnp.clip(large + rough, -512.0, 512.0)
    return values.reshape(M, B, D)


def draw_weights(key, part):
    basis_cols = shared_basis(key)
    matrices = []
    for level in range(LAYERS):
        layer_key = jax.random.fold_in(key, 401 + level)
        dense = jnp.clip(jax.random.normal(layer_key, (D, D), jnp.float32), -6.0, 6.0) / math.sqrt(D)
        inside = jnp.dot(basis_cols.T, dense, precision=lax.Precision.HIGHEST)
        matrix = dense - (1.0 - 1.0 / offset_scale) * jnp.dot(basis_cols, inside, precision=lax.Precision.HIGHEST)
        matrices.append(matrix.reshape(ROW_BLOCKS, COL_BLOCKS, PIECE, D))
    return jnp.stack(matrices)


def setup_inputs(seed: int = 0) -> dict:
    key_of = jax.random.split(jax.random.key(seed), 4)
    return {
        "inputs": draw_inputs(jax.random.fold_in(key_of[3], 71), 0),
        "weights": draw_weights(jax.random.fold_in(key_of[3], 71), 0),
        "norm_gain": jnp.clip(1.0 + 0.1 * jax.random.normal(key_of[2], (LAYERS, D), jnp.float32), 0.5, 1.5),
    }


def split_two(values):
    first = lax.optimization_barrier(values.astype(jnp.bfloat16))
    second = lax.optimization_barrier((values - first.astype(jnp.float32)).astype(jnp.bfloat16))
    return (first, second)

def widen(values):
    return values.astype(jnp.float32)

def layer(activations, matrix, gain):
    first, second = split_two(activations)
    sum_two = widen(first) + widen(second)
    sum_one = widen(first)
    width = matrix.shape[1]
    block_cols = width // 8

    def column_block(index):
        cols = lax.dynamic_slice_in_dim(matrix, (index * block_cols).astype(jnp.int32), block_cols, 1)
        wfirst, wsecond = split_two(cols)
        total = jnp.dot(sum_two.astype(jnp.float32), widen(wfirst).astype(jnp.float32), precision=lax.Precision.HIGHEST, preferred_element_type=jnp.float32)
        total = total + jnp.dot(sum_one.astype(jnp.float32), widen(wsecond).astype(jnp.float32), precision=lax.Precision.HIGHEST, preferred_element_type=jnp.float32)
        return total
    blocks = lax.map(column_block, jnp.arange(8, dtype=jnp.int32))
    summed = jnp.transpose(blocks, (1, 0, 2)).reshape(activations.shape[0], width)
    active = jax.nn.gelu(summed, approximate=True)
    squares = lax.optimization_barrier(jnp.sum(active * active, axis=1))
    scale = lax.rsqrt(squares / width + 1e-06)
    return active * scale[:, None] * gain[None, :]

def reference(inputs, weights, norm_gain):
    current = inputs.reshape(M * B, D)
    results = []
    for level in range(LAYERS):
        matrix = weights[level].reshape(D, D)
        branch = layer(current, matrix, norm_gain[level])
        results.append(branch.reshape(M, B, D))
        current = current + branch
    return jnp.stack(results)
```

```python
import functools

import jax
import jax.numpy as jnp
from jax import lax
from jax.experimental import pallas as pl
from jax.experimental.pallas import tpu as pltpu
from jax.sharding import PartitionSpec as P

MESH = pl.DeviceIdType.MESH
GROUP = 16
SLOTS = 4


def slices(values):
    first = values.astype(jnp.bfloat16)
    second = (values - first.astype(jnp.float32)).astype(jnp.bfloat16)
    return first, second


def kernel(
    sections, row_count, col_count,
    x_ref, w_ref, gain_ref, out_ref,
    gathered, lhs, part, landed, active, squares, handed, handing, tiles,
    col_out, col_in, row_out, row_in,
    tile_sem, ag_send, ag_recv, rs_send, rs_recv,
    col_send, col_recv, row_send, row_recv, next_send, next_recv,
):
    micro, rows, pieces = x_ref.shape
    width = tiles.shape[2]
    per_chunk = pieces // width
    per_micro = per_chunk * col_count
    total_features = pieces * row_count * col_count
    section = lax.axis_index("section")
    row = lax.axis_index("row")
    col = lax.axis_index("col")
    cores = 2 if row_count % 2 == 0 else 1
    chips = row_count // cores
    core = lax.rem(row, cores)
    chip = row // cores

    def around(position, step, count):
        return lax.rem(position + step, count)

    def chip_row(step, which):
        return around(chip, step, chips) * cores + which

    def remote(src, dst, send, recv, device):
        return pltpu.make_async_remote_copy(
            src_ref=src, dst_ref=dst, send_sem=send, recv_sem=recv,
            device_id=device, device_id_type=MESH,
        )

    def fetch(step):
        within = lax.rem(step, per_micro)
        chunk = around(col, 1 + within // per_chunk, col_count)
        start = chunk * pieces + lax.rem(within, per_chunk) * width
        slot = lax.rem(step, SLOTS)
        return pltpu.make_async_copy(
            w_ref.at[:, pl.ds(pl.multiple_of(start, width), width)],
            tiles.at[slot], tile_sem.at[slot],
        )

    for step in range(SLOTS - 1):
        fetch(step).start()

    barrier = pltpu.get_barrier_semaphore()
    for step in range(1, row_count):
        pl.semaphore_signal(barrier, inc=1, device_id={"row": around(row, step, row_count)}, device_id_type=MESH)
    for step in range(1, col_count):
        pl.semaphore_signal(barrier, inc=1, device_id={"col": around(col, step, col_count)}, device_id_type=MESH)

    @pl.when(section > 0)
    def _():
        pl.semaphore_signal(barrier, inc=1, device_id={"section": section - 1}, device_id_type=MESH)

    @pl.when(section < sections - 1)
    def _():
        pl.semaphore_signal(barrier, inc=1, device_id={"section": section + 1}, device_id_type=MESH)

    before = (section + sections - 1) // sections
    after = (2 * (sections - 1) - section) // sections
    pl.semaphore_wait(barrier, row_count + col_count - 2 + before + after)

    def gather_send(m, source, target):
        return remote(source, gathered.at[m, row], ag_send.at[m, target], ag_recv.at[m, row], {"row": target})

    def gather_start(m, source):
        gathered[m, row] = source[...]
        for step in range(1, chips):
            gather_send(m, source, chip_row(step, core)).start()
        if cores == 2:
            gather_send(m, source, chip * cores + 1 - core).start()

    def gather_forward(m, step):
        held = chip_row(step, core)
        slot = chip_row(step, 1 - core)
        return remote(
            gathered.at[m, held], gathered.at[m, held], ag_send.at[m, slot],
            ag_recv.at[m, held], {"row": chip * cores + 1 - core},
        )

    def gather_landed(m, source):
        target = around(row, 1, row_count)
        remote(gathered.at[m, source], gathered.at[m, source], ag_send.at[m, source],
               ag_recv.at[m, source], {"row": target}).wait_recv()

    def hand(m):
        return remote(handing.at[m], handed.at[m], next_send.at[m], next_recv.at[m], {"section": section + 1})

    def chunk_send(m, chunk):
        return remote(part.at[m, chunk], landed.at[m, col], rs_send.at[m, chunk], rs_recv.at[m, col], {"col": chunk})

    @pl.when(section == 0)
    def _():
        def begin(m, carry):
            gather_start(m, x_ref.at[m])
            return carry
        lax.fori_loop(0, micro, begin, 0)

    def multiply(m):
        @pl.when(section > 0)
        def _():
            remote(handing.at[m], handed.at[m], next_send.at[m], next_recv.at[m], {"section": section - 1}).wait_recv()
            gather_start(m, handed.at[m])

        for step in range(1, chips):
            gather_landed(m, chip_row(step, core))
            if cores == 2:
                gather_forward(m, step).start()
        if cores == 2:
            for step in range(chips):
                gather_landed(m, chip_row(step, 1 - core))

        def prepare(r, carry):
            first, second = slices(gathered[m, r])
            lhs[r, :rows] = first
            lhs[r, rows:] = second
            return carry
        lax.fori_loop(0, row_count, prepare, 0)

        def chunk_body(i, carry):
            chunk = around(col, 1 + i, col_count)

            def tile_body(j, carry):
                step = m * per_micro + i * per_chunk + j
                slot = lax.rem(step, SLOTS)

                @pl.when(step + SLOTS - 1 < micro * per_micro)
                def _():
                    fetch(step + SLOTS - 1).start()

                fetch(step).wait()
                both = jnp.zeros((2 * rows, width), jnp.float32)
                low = jnp.zeros((rows, width), jnp.float32)
                for r in range(row_count):
                    first, second = slices(tiles[slot, r * pieces:(r + 1) * pieces, :])
                    both += jnp.dot(lhs[r], first, preferred_element_type=jnp.float32)
                    low += jnp.dot(lhs[r, :rows], second, preferred_element_type=jnp.float32)
                part[m, chunk, :, pl.ds(pl.multiple_of(j * width, width), width)] = both[:rows] + (both[rows:] + low)
                return carry
            lax.fori_loop(0, per_chunk, tile_body, 0)

            @pl.when(i < col_count - 1)
            def _():
                chunk_send(m, chunk).start()
            return carry
        lax.fori_loop(0, col_count, chunk_body, 0)

    def finish(m):
        for step in range(1, col_count):
            source = around(col, step, col_count)
            remote(part.at[m, source], landed.at[m, source], rs_send.at[m, source],
                   rs_recv.at[m, source], {"col": source}).wait_recv()

        def activate(g, carry):
            span = pl.ds(pl.multiple_of(g * GROUP, GROUP), GROUP)
            z = part[m, col, span, :]
            for step in range(1, col_count):
                z += landed[m, around(col, step, col_count), span, :]
            y = jax.nn.gelu(z, approximate=True)
            active[span, :] = y
            squares[span, :] = jnp.broadcast_to(jnp.sum(y * y, axis=1, keepdims=True), (GROUP, 128))
            return carry
        lax.fori_loop(0, rows // GROUP, activate, 0)

        def share(own, outgoing, incoming, send, recv, axis, position, count):
            outgoing[m] = own
            copies = []
            for step in range(1, count):
                target = around(position, step, count)
                copies.append(remote(outgoing.at[m], incoming.at[m, position], send.at[m, target],
                                     recv.at[m, position], {axis: target}))
                copies[-1].start()
            total = own
            for step in range(1, count):
                source = around(position, step, count)
                remote(outgoing.at[m], incoming.at[m, source], send.at[m, source],
                       recv.at[m, source], {axis: source}).wait_recv()
                total = total + incoming[m, source]
            for copy in copies:
                copy.wait_send()
            return total

        total = squares[...].T[:8]
        total = share(total, col_out, col_in, col_send, col_recv, "col", col, col_count)
        total = share(total, row_out, row_in, row_send, row_recv, "row", row, row_count)
        scale = lax.rsqrt(total[:1] / total_features + 1e-06)
        squares[...] = jnp.broadcast_to(scale, (128, rows)).T

        def normalize(g, carry):
            span = pl.ds(pl.multiple_of(g * GROUP, GROUP), GROUP)
            o = active[span, :] * squares[span, :1] * gain_ref[...]
            out_ref[m, span, :] = o
            handing[m, span, :] = gathered[m, row, span, :] + o
            return carry
        lax.fori_loop(0, rows // GROUP, normalize, 0)

        @pl.when(section < sections - 1)
        def _():
            hand(m).start()

    def step_body(m, carry):
        @pl.when(m < micro)
        def _():
            multiply(m)

        @pl.when(m > 0)
        def _():
            finish(m - 1)
        return carry
    lax.fori_loop(0, micro + 1, step_body, 0)

    def drain(m, carry):
        for step in range(1, chips):
            gather_send(m, x_ref.at[m], chip_row(step, core)).wait_send()
            if cores == 2:
                gather_forward(m, step).wait_send()
        if cores == 2:
            gather_send(m, x_ref.at[m], chip * cores + 1 - core).wait_send()
        for step in range(1, col_count):
            chunk_send(m, around(col, step, col_count)).wait_send()

        @pl.when(section < sections - 1)
        def _():
            hand(m).wait_send()
        return carry
    lax.fori_loop(0, micro, drain, 0)


def solution(mesh):
    sections, row_count, col_count = (mesh.shape[name] for name in ("section", "row", "col"))

    def shards(inputs, weights, norm_gain):
        micro, rows, pieces = inputs.shape
        depth = row_count * pieces
        out_cols = weights.shape[4]
        width = min(256, pieces)
        f32 = jnp.float32
        dma = pltpu.SemaphoreType.DMA
        result = pl.pallas_call(
            functools.partial(kernel, sections, row_count, col_count),
            out_shape=jax.ShapeDtypeStruct((micro, rows, pieces), f32),
            in_specs=[
                pl.BlockSpec(memory_space=pltpu.VMEM),
                pl.BlockSpec(memory_space=pltpu.HBM),
                pl.BlockSpec(memory_space=pltpu.VMEM),
            ],
            out_specs=pl.BlockSpec(memory_space=pltpu.VMEM),
            scratch_shapes=[
                pltpu.VMEM((micro, row_count, rows, pieces), f32),
                pltpu.VMEM((row_count, 2 * rows, pieces), jnp.bfloat16),
                pltpu.VMEM((micro, col_count, rows, pieces), f32),
                pltpu.VMEM((micro, col_count, rows, pieces), f32),
                pltpu.VMEM((rows, pieces), f32),
                pltpu.VMEM((rows, 128), f32),
                pltpu.VMEM((micro, rows, pieces), f32),
                pltpu.VMEM((micro, rows, pieces), f32),
                pltpu.VMEM((SLOTS, depth, width), f32),
                pltpu.VMEM((micro, 8, rows), f32),
                pltpu.VMEM((micro, col_count, 8, rows), f32),
                pltpu.VMEM((micro, 8, rows), f32),
                pltpu.VMEM((micro, row_count, 8, rows), f32),
                dma((SLOTS,)),
                dma((micro, row_count)),
                dma((micro, row_count)),
                dma((micro, col_count)),
                dma((micro, col_count)),
                dma((micro, col_count)),
                dma((micro, col_count)),
                dma((micro, row_count)),
                dma((micro, row_count)),
                dma((micro,)),
                dma((micro,)),
            ],
            compiler_params=pltpu.CompilerParams(
                collective_id=0, has_side_effects=True, vmem_limit_bytes=60 * 1024 * 1024
            ),
        )(inputs, weights.reshape(depth, out_cols), norm_gain)
        return result[None]

    placed = (
        P(None, None, ("row", "col")),
        P("section", None, "col", None, "row"),
        P("section", ("row", "col")),
    )
    return jax.shard_map(
        shards,
        mesh=mesh,
        in_specs=placed,
        out_specs=P("section", None, None, ("row", "col")),
        check_vma=False,
    )
```
